8 devices in a mesh: dp: 1 (over z), tp: 2 (over y), sp: 4 (over x, core).
Axes of the slice: x: 2, y: 2, z: 1, core: 2. Of those that a mesh axis runs over, the one named last changes fastest.
Arguments:
- feats: bfloat16 [64, 4096, 1152], P(('dp', 'sp'))
- tokens: int32 [32768], P(('dp', 'sp'))
- img_slot: int32 [32768], P(('dp', 'sp'))
- img_id: int32 [32768], P(('dp', 'sp'))
- embed: bfloat16 [16384, 2560], P('tp')
- proj_norm: float32 [1152], replicated
- w_proj: bfloat16 [1152, 2560], replicated
- norms: float32 [4, 2560], replicated
- qk_norms: float32 [2, 256], replicated
- w_q: bfloat16 [2560, 2048], P(None, 'tp')
- w_k: bfloat16 [2560, 1024], P(None, 'tp')
- w_v: bfloat16 [2560, 1024], P(None, 'tp')
- w_o: bfloat16 [2048, 2560], P('tp')
- w_gate: bfloat16 [2560, 10240], P(None, 'tp')
- w_up: bfloat16 [2560, 10240], P(None, 'tp')
- w_down: bfloat16 [10240, 2560], P('tp')
Outputs:
- output: bfloat16 [32768, 2560], P(('dp', 'sp'))
All inputs are finite; a program needn't handle non-finite values.
Results may differ from the reference program's by a relative error of at most 0.0182194.
Values are sent between devices in bfloat16 or wider.
A program may use at most 1.25 GiB of HBM per device.

```python
import jax
import jax.numpy as jnp
from jax import lax

D_MODEL = 2560
HEADS = 8
KV_HEADS = 4
HEAD_DIM = 256
FF_DIM = 10240
VOCAB = 16384
SEQ_LEN = 32768
SHARD_LEN = 8192
NUM_IMG = 64
WINDOW = 1024
VIS_DIM = 1152
PATCHES = 4096
SOFT_PER_IMG = 256
POOL_SIDE = 16
POOL_K = 4
BLOCK_Q = 256
ROW_BLOCK = 1024

EPS = 1e-6
ROPE_BASE = 10000.0


def draw_layout(layout_key):
    perm_key, gap_key = jax.random.split(layout_key)
    order = jax.random.permutation(perm_key, NUM_IMG).astype(jnp.int32)
    first_gap = SHARD_LEN - SOFT_PER_IMG // 2
    spare = SEQ_LEN - NUM_IMG * SOFT_PER_IMG - first_gap
    weights = jax.random.randint(gap_key, (NUM_IMG,), 0, 16, jnp.int32) ** 2
    gaps = spare * weights // (jnp.sum(weights) + 1)
    starts = first_gap + SOFT_PER_IMG * jnp.arange(NUM_IMG, dtype=jnp.int32) + jnp.cumsum(gaps) - gaps
    positions = jnp.arange(SEQ_LEN, dtype=jnp.int32)
    marks = jnp.zeros((SEQ_LEN,), jnp.int32).at[starts].add(1)
    run_index = jnp.cumsum(marks) - 1
    safe_run = jnp.maximum(run_index, 0)
    offset = positions - starts[safe_run]
    inside = (run_index >= 0) & (offset < SOFT_PER_IMG)
    image_of = order[safe_run]
    img_id = jnp.where(inside, image_of, -1)
    img_slot = jnp.where(inside, image_of * SOFT_PER_IMG + offset, -1)
    return img_slot.astype(jnp.int32), img_id.astype(jnp.int32)


def normal_draw(draw_key, shape, scale):
    return jax.random.normal(draw_key, shape, jnp.float32) * scale


def draw_table(draw_key, scale):
    block_keys = jax.random.split(draw_key, VOCAB // 1024)

    def one_block(block_key):
        return (jax.random.normal(block_key, (1024, D_MODEL), jnp.float32) * scale).astype(jnp.bfloat16)

    return lax.map(one_block, block_keys).reshape(VOCAB, D_MODEL)


def setup_inputs(seed: int = 0, part: int = 0) -> dict:
    base_key = jax.random.key(seed)
    part_key = jax.random.fold_in(base_key, part)
    part_keys = jax.random.split(part_key, 3)
    shared = jax.random.split(base_key, 12)

    def draw_image(img_key):
        return jax.random.normal(img_key, (PATCHES, VIS_DIM), jnp.float32).astype(jnp.bfloat16)

    feats = lax.map(draw_image, jax.random.split(part_keys[0], NUM_IMG))
    tokens = jax.random.randint(part_keys[1], (SEQ_LEN,), 0, VOCAB, jnp.int32)
    img_slot, img_id = draw_layout(part_keys[2])
    return {
        'feats': feats,
        'tokens': tokens,
        'img_slot': img_slot,
        'img_id': img_id,
        'embed': draw_table(shared[0], D_MODEL ** -0.5),
        'proj_norm': normal_draw(shared[1], (VIS_DIM,), 0.5),
        'w_proj': normal_draw(shared[2], (VIS_DIM, D_MODEL), VIS_DIM ** -0.5).astype(jnp.bfloat16),
        'norms': normal_draw(shared[3], (4, D_MODEL), 0.5),
        'qk_norms': normal_draw(shared[4], (2, HEAD_DIM), 0.5),
        'w_q': normal_draw(shared[5], (D_MODEL, HEADS * HEAD_DIM), D_MODEL ** -0.5).astype(jnp.bfloat16),
        'w_k': normal_draw(shared[6], (D_MODEL, KV_HEADS * HEAD_DIM), D_MODEL ** -0.5).astype(jnp.bfloat16),
        'w_v': normal_draw(shared[7], (D_MODEL, KV_HEADS * HEAD_DIM), D_MODEL ** -0.5).astype(jnp.bfloat16),
        'w_o': normal_draw(shared[8], (HEADS * HEAD_DIM, D_MODEL), (HEADS * HEAD_DIM) ** -0.5).astype(jnp.bfloat16),
        'w_gate': normal_draw(shared[9], (D_MODEL, FF_DIM), D_MODEL ** -0.5).astype(jnp.bfloat16),
        'w_up': normal_draw(shared[10], (D_MODEL, FF_DIM), D_MODEL ** -0.5).astype(jnp.bfloat16),
        'w_down': normal_draw(shared[11], (FF_DIM, D_MODEL), FF_DIM ** -0.5).astype(jnp.bfloat16),
    }


def rms_norm(values, weight):
    wide = values.astype(jnp.float32)
    mean_sq = jnp.mean(wide * wide, axis=-1, keepdims=True)
    return wide * lax.rsqrt(mean_sq + EPS) * (1.0 + weight)


def rope_tables(positions):
    half_dim = HEAD_DIM // 2
    inv_freq = jnp.power(ROPE_BASE, -2.0 * jnp.arange(half_dim, dtype=jnp.float32) / HEAD_DIM)
    angles = positions.astype(jnp.float32)[:, None] * inv_freq[None, :]
    return jnp.cos(angles), jnp.sin(angles)


def apply_rope(values, cos_t, sin_t):
    half_dim = values.shape[-1] // 2
    lower = values[..., :half_dim]
    upper = values[..., half_dim:]
    cos_b = cos_t[:, None, :]
    sin_b = sin_t[:, None, :]
    return jnp.concatenate([lower * cos_b - upper * sin_b, upper * cos_b + lower * sin_b], axis=-1)


def reference(feats, tokens, img_slot, img_id, embed, proj_norm, w_proj, norms, qk_norms, w_q, w_k, w_v, w_o, w_gate, w_up, w_down):
    def soft_of_image(image):
        grouped = image.astype(jnp.float32).reshape(POOL_SIDE, POOL_K, POOL_SIDE, POOL_K, VIS_DIM)
        pooled = jnp.mean(grouped, axis=(1, 3)).reshape(SOFT_PER_IMG, VIS_DIM)
        normed = rms_norm(pooled, proj_norm).astype(jnp.bfloat16)
        return jnp.dot(normed, w_proj, preferred_element_type=jnp.float32).astype(jnp.bfloat16)

    soft = lax.map(soft_of_image, feats).reshape(NUM_IMG * SOFT_PER_IMG, D_MODEL)
    scale = jnp.sqrt(jnp.float32(D_MODEL)).astype(jnp.bfloat16).astype(jnp.float32)
    text_emb = (jnp.take(embed, tokens, axis=0).astype(jnp.float32) * scale).astype(jnp.bfloat16)
    soft_rows = jnp.take(soft, jnp.maximum(img_slot, 0), axis=0)
    x_in = jnp.where(img_slot[:, None] >= 0, soft_rows, text_emb)

    n_rows = SEQ_LEN // ROW_BLOCK
    groups = HEADS // KV_HEADS

    def project_rows(block):
        x_blk = lax.dynamic_slice_in_dim(x_in, block * ROW_BLOCK, ROW_BLOCK, 0)
        cos_t, sin_t = rope_tables(block * ROW_BLOCK + jnp.arange(ROW_BLOCK))
        normed = rms_norm(x_blk, norms[0]).astype(jnp.bfloat16)
        query = jnp.dot(normed, w_q, preferred_element_type=jnp.float32).reshape(ROW_BLOCK, HEADS, HEAD_DIM)
        query = apply_rope(rms_norm(query, qk_norms[0]), cos_t, sin_t).astype(jnp.bfloat16)
        key_blk = jnp.dot(normed, w_k, preferred_element_type=jnp.float32).reshape(ROW_BLOCK, KV_HEADS, HEAD_DIM)
        key_blk = apply_rope(rms_norm(key_blk, qk_norms[1]), cos_t, sin_t).astype(jnp.bfloat16)
        value_blk = jnp.dot(normed, w_v, preferred_element_type=jnp.float32).astype(jnp.bfloat16).reshape(ROW_BLOCK, KV_HEADS, HEAD_DIM)
        return query, key_blk, value_blk

    query_all, key_all, value_all = lax.map(project_rows, jnp.arange(n_rows))
    q_blocks = query_all.reshape(SEQ_LEN // BLOCK_Q, BLOCK_Q, KV_HEADS, groups, HEAD_DIM)
    key_pad = jnp.pad(key_all.reshape(SEQ_LEN, KV_HEADS, HEAD_DIM), ((WINDOW, SOFT_PER_IMG), (0, 0), (0, 0)))
    value_pad = jnp.pad(value_all.reshape(SEQ_LEN, KV_HEADS, HEAD_DIM), ((WINDOW, SOFT_PER_IMG), (0, 0), (0, 0)))
    id_pad = jnp.pad(img_id, (WINDOW, SOFT_PER_IMG), constant_values=-1)
    span = WINDOW + BLOCK_Q + SOFT_PER_IMG

    def attend(block):
        start = block * BLOCK_Q
        q_blk = q_blocks[block].astype(jnp.float32)
        k_blk = lax.dynamic_slice_in_dim(key_pad, start, span, 0).astype(jnp.float32)
        v_blk = lax.dynamic_slice_in_dim(value_pad, start, span, 0).astype(jnp.float32)
        q_ids = lax.dynamic_slice_in_dim(img_id, start, BLOCK_Q, 0)
        k_ids = lax.dynamic_slice_in_dim(id_pad, start, span, 0)
        q_pos = start + jnp.arange(BLOCK_Q)
        k_pos = start - WINDOW + jnp.arange(span)
        distance = q_pos[:, None] - k_pos[None, :]
        same_img = (q_ids[:, None] == k_ids[None, :]) & (q_ids[:, None] >= 0)
        allowed = (((distance >= 0) & (distance < WINDOW)) | same_img) & (k_pos[None, :] >= 0) & (k_pos[None, :] < SEQ_LEN)
        scores = jnp.einsum('qkgd,lkd->kgql', q_blk, k_blk) * HEAD_DIM ** -0.5
        scores = jnp.where(allowed[None, None], scores, -1e30)
        attn_weights = jax.nn.softmax(scores, axis=-1).astype(jnp.bfloat16).astype(jnp.float32)
        mixed = jnp.einsum('kgql,lkd->qkgd', attn_weights, v_blk)
        return mixed.astype(jnp.bfloat16).reshape(BLOCK_Q, HEADS * HEAD_DIM)

    attn = lax.map(attend, jnp.arange(SEQ_LEN // BLOCK_Q)).reshape(SEQ_LEN, HEADS * HEAD_DIM)

    def finish_rows(block):
        x_blk = lax.dynamic_slice_in_dim(x_in, block * ROW_BLOCK, ROW_BLOCK, 0)
        a_blk = lax.dynamic_slice_in_dim(attn, block * ROW_BLOCK, ROW_BLOCK, 0)
        attn_out = jnp.dot(a_blk, w_o, preferred_element_type=jnp.float32).astype(jnp.bfloat16)
        post = rms_norm(attn_out, norms[1]).astype(jnp.bfloat16)
        hidden = (x_blk.astype(jnp.float32) + post.astype(jnp.float32)).astype(jnp.bfloat16)
        ffn_in = rms_norm(hidden, norms[2]).astype(jnp.bfloat16)
        gate = jnp.dot(ffn_in, w_gate, preferred_element_type=jnp.float32)
        up_proj = jnp.dot(ffn_in, w_up, preferred_element_type=jnp.float32)
        activated = (jax.nn.gelu(gate, approximate=True) * up_proj).astype(jnp.bfloat16)
        down = jnp.dot(activated, w_down, preferred_element_type=jnp.float32).astype(jnp.bfloat16)
        ffn_post = rms_norm(down, norms[3]).astype(jnp.bfloat16)
        return (hidden.astype(jnp.float32) + ffn_post.astype(jnp.float32)).astype(jnp.bfloat16)

    return lax.map(finish_rows, jnp.arange(n_rows)).reshape(SEQ_LEN, D_MODEL)
```

```python
import functools

import jax
import jax.numpy as jnp
import numpy as np
from jax import lax
from jax.experimental import pallas as pl
from jax.experimental.pallas import tpu as pltpu
from jax.sharding import PartitionSpec as P

BF = jnp.bfloat16
F32 = jnp.float32
EPS = 1e-6
ROPE_BASE = 10000.0
WINDOW = 1024
SOFT = 256
HD = 256
VMEM_LIMIT = 67_000_000


ANY = pl.BlockSpec(memory_space=pl.ANY)
DMA = pltpu.SemaphoreType.DMA


def params(**kw):
    return pltpu.CompilerParams(vmem_limit_bytes=VMEM_LIMIT, **kw)


def cost(macs, nbytes):
    return pl.CostEstimate(flops=2 * macs, bytes_accessed=nbytes, transcendentals=0)


def by_row(i, *_):
    return (i, 0)


def fixed(*_):
    return (0, 0)


def whole(shape):
    return pl.BlockSpec(shape, fixed, pipeline_mode=pl.Buffered(1))


def like(shape, dtype=BF):
    return jax.ShapeDtypeStruct(shape, dtype)


def normed(values, weight):
    mean_sq = jnp.mean(values * values, axis=-1, keepdims=True)
    return values * lax.rsqrt(mean_sq + EPS) * (1.0 + weight)


POOL_GROUPS = 4
POOL_K = 4
PATCH_SIDE = 64
E_START = 150_000_000_000


def gather_kernel(feats, embed, pn_ref, pmat_ref, idx_ref, w_q, w_k, w_v, w_o, w_g, w_u, w_d,
                  table, pooled, idx_all, qkv_p, o_p, g_p, u_p, d_p,
                  f_buf, p_buf, c_buf, i_buf, qkv_b, o_b, g_b, u_b, d_b,
                  f_sem, p_sem, c_in, c_out, w_in, w_out, ys, yr, xs, xr, gs, gr, ts, tr, os, orr, rs, rr, ns, nr, i_sem):
    tp = lax.axis_index("tp")
    sp = lax.axis_index("sp")
    x = sp // 2
    c = sp % 2
    other_x = sp ^ 2
    ypeer, xpeer, cpeer, dpeer = {"tp": 1 - tp}, {"sp": other_x}, {"sp": sp ^ 1}, {"sp": other_x ^ 1}
    mesh_id = pl.DeviceIdType.MESH
    n_img = feats.shape[0]
    vocab = embed.shape[0]
    quarter = vocab // 4
    part = quarter // 2
    bar = pltpu.get_barrier_semaphore()
    for peer in (ypeer, xpeer, cpeer, dpeer):
        pl.semaphore_signal(bar, inc=1, device_id=peer, device_id_type=mesh_id)
    pl.semaphore_wait(bar, 4)

    def remote(src, dst, s, r, peer):
        return pltpu.make_async_remote_copy(src_ref=src, dst_ref=dst, send_sem=s, recv_sem=r, device_id=peer, device_id_type=mesh_id)

    def part_row(xx, p):
        q = 3 * xx if p == 0 else p
        return q * quarter + c * part

    def rows(start, size):
        return pl.ds(pl.multiple_of(start, 256), size)

    mine = tp * vocab
    other = (1 - tp) * vocab
    y_copies = []
    for p in range(3):
        r0 = part_row(x, p)
        cp = remote(embed.at[rows(r0, part), :], table.at[rows(mine + r0, part), :], ys.at[p], yr.at[p], ypeer)
        cp.start()
        y_copies.append(cp)

    n_tok = idx_ref.shape[1]
    here = idx_all.at[:, rows(sp * n_tok, n_tok)]
    n_copies = [remote(idx_ref, here, ns.at[k], nr.at[k], peer) for k, peer in enumerate((xpeer, cpeer, dpeer))]
    for cp in n_copies:
        cp.start()

    def load(n, slot):
        return pltpu.make_async_copy(feats.at[n], f_buf.at[slot], f_sem.at[slot])

    load(0, 0).start()

    def cut(k, size):
        return pl.ds(pl.multiple_of(sp * size, size), size)

    e = w_q.shape[0] // 4
    nq, nk = w_q.shape[1], w_k.shape[1]
    cuts = [(w_q.at[cut(0, e), :], qkv_b.at[:, 0:nq]), (w_k.at[cut(0, e), :], qkv_b.at[:, nq:nq + nk]), (w_v.at[cut(0, e), :], qkv_b.at[:, nq + nk:]),
            (w_o.at[cut(0, w_o.shape[0] // 4), :], o_b), (w_g.at[cut(0, e), :], g_b), (w_u.at[cut(0, e), :], u_b), (w_d.at[:, cut(0, e)], d_b)]
    w_loads = [pltpu.make_async_copy(src, dst, w_in.at[k]) for k, (src, dst) in enumerate(cuts)]
    w_stores = [pltpu.make_async_copy(src, dst, w_out.at[k]) for k, (src, dst) in enumerate(((qkv_b, qkv_p), (o_b, o_p), (g_b, g_p), (u_b, u_p), (d_b, d_p)))]

    per = n_img // POOL_GROUPS
    own = sp * n_img * SOFT
    side = pmat_ref.shape[1]
    x_copies, o_copies = [], []
    for g in range(POOL_GROUPS):
        def one(k, carry):
            n = g * per + k
            slot = lax.rem(n, 2)

            @pl.when(n + 1 < n_img)
            def _():
                load(n + 1, 1 - slot).start()

            load(n, slot).wait()
            for r in range(16):
                acc = jnp.dot(pmat_ref[...], f_buf[slot, r * side:(r + 1) * side, :], preferred_element_type=F32)
                p_buf[pl.ds(pl.multiple_of(k * SOFT + r * 16, 16), 16), :] = normed(acc, pn_ref[...]).astype(BF)
            return carry

        lax.fori_loop(0, per, one, 0)
        size = per * SOFT
        dst = pooled.at[rows(own + g * size, size), :]
        put = pltpu.make_async_copy(p_buf, dst, p_sem)
        put.start()
        put.wait()
        cx = remote(dst, dst, xs.at[g], xr.at[g], xpeer)
        co = remote(dst, dst, os.at[g], orr.at[g], cpeer)
        cx.start()
        co.start()
        x_copies.append(cx)
        o_copies.append(co)

    for cp in w_loads:
        cp.start()

    step = c_buf.shape[1]
    n_step = vocab // step

    def c_load(i, slot):
        return pltpu.make_async_copy(embed.at[rows(i * step, step), :], c_buf.at[slot], c_in.at[slot])

    def c_store(i, slot):
        return pltpu.make_async_copy(c_buf.at[slot], table.at[rows(mine + i * step, step), :], c_out.at[slot])

    c_load(0, 0).start()

    def copy_step(i, carry):
        slot = lax.rem(i, 2)

        @pl.when(i + 1 < n_step)
        def _():
            @pl.when(i >= 1)
            def _():
                c_store(i - 1, 1 - slot).wait()
            c_load(i + 1, 1 - slot).start()

        c_load(i, slot).wait()
        c_store(i, slot).start()
        return carry

    lax.fori_loop(0, n_step, copy_step, 0)
    for i in (n_step - 2, n_step - 1):
        c_store(i, i % 2).wait()
    for cp in w_loads:
        cp.wait()
    for cp in w_stores:
        cp.start()
    get = pltpu.make_async_copy(idx_ref, i_buf, i_sem)
    get.start()
    get.wait()
    put = pltpu.make_async_copy(i_buf, here, i_sem)
    put.start()
    put.wait()

    size = per * SOFT
    xown = other_x * n_img * SOFT
    r_copies, t_copies = [], []

    def relay_pooled(g):
        x_copies[g].wait_recv()
        ref = pooled.at[rows(xown + g * size, size), :]
        cp = remote(ref, ref, rs.at[g], rr.at[g], cpeer)
        cp.start()
        r_copies.append(cp)

    def relay_table(r0, k):
        ref = table.at[rows(other + r0, part), :]
        cp = remote(ref, ref, ts.at[k], tr.at[k], cpeer)
        cp.start()
        t_copies.append(cp)

    relay_pooled(0)
    y_copies[0].wait_recv()
    ref = table.at[rows(other + part_row(x, 0), part), :]
    cg = remote(ref, ref, gs, gr, xpeer)
    cg.start()
    relay_table(part_row(x, 0), 0)
    for g in range(1, POOL_GROUPS):
        relay_pooled(g)
    y_copies[1].wait_recv()
    relay_table(part_row(x, 1), 1)
    cg.wait_recv()
    relay_table(part_row(1 - x, 0), 2)
    y_copies[2].wait_recv()
    relay_table(part_row(x, 2), 3)
    for cp in n_copies + o_copies + r_copies + t_copies:
        cp.wait_recv()
    for cp in y_copies + x_copies + n_copies + o_copies + r_copies + t_copies + [cg]:
        cp.wait_send()
    for cp in w_stores:
        cp.wait()


def gather_inputs(feats, embed, proj_norm, pmat, idx, *weights):
    n_img, patches, vis = feats.shape
    vocab, d = embed.shape
    w_q, w_k, w_v, w_o, w_g, w_u, w_d = weights
    n4 = DMA((POOL_GROUPS,))
    vmem = pl.BlockSpec(memory_space=pltpu.VMEM)
    e = d // 4
    cuts = [(e, w_q.shape[1] + 2 * w_k.shape[1]), (w_o.shape[0] // 4, d), (e, w_g.shape[1]), (e, w_u.shape[1]), (w_d.shape[0], e)]
    out_shape = [like((2 * vocab, d), BF), like((4 * n_img * SOFT, vis), BF), like((8, 4 * idx.shape[1]), jnp.int32)]
    out_shape += [like(c, BF) for c in cuts]
    return pl.pallas_call(
        gather_kernel,
        in_specs=[ANY, ANY, vmem, vmem] + [ANY] * 8,
        out_specs=[ANY] * len(out_shape),
        out_shape=out_shape,
        scratch_shapes=[
            pltpu.VMEM((2, patches, vis), BF), pltpu.VMEM((n_img // POOL_GROUPS * SOFT, vis), BF), pltpu.VMEM((2, 512, d), BF), pltpu.VMEM(idx.shape, jnp.int32),
            *[pltpu.VMEM(c, BF) for c in cuts],
            DMA((2,)), DMA, DMA((2,)), DMA((2,)), DMA((7,)), DMA((5,)),
            DMA((3,)), DMA((3,)), n4, n4, DMA, DMA, DMA((4,)), DMA((4,)), n4, n4, n4, n4, DMA((3,)), DMA((3,)), DMA],
        compiler_params=params(collective_id=0, has_side_effects=True),
        cost_estimate=cost(E_START, feats.size),
        name="gather_inputs",
    )(feats, embed, proj_norm, pmat, idx, *weights)


IMG = 65536
ROW_BLOCK = 128


def index_rows(tokens, img_slot, img_id):
    one = (img_slot >= 0).astype(jnp.int32)
    row = jnp.where(img_slot >= 0, img_slot, tokens)
    count = jnp.sum(one.reshape(-1, ROW_BLOCK), axis=1, keepdims=True)
    count = jnp.broadcast_to(count, (count.shape[0], ROW_BLOCK)).reshape(-1)
    return jnp.stack([row // 8 * 8 + IMG * one, row % 8 + 8 * one, img_id, count] + [jnp.zeros_like(row)] * 4)


def as_column(row):
    wide = jnp.broadcast_to(row.astype(F32), (8, row.shape[1]))
    return wide.T[:, 0:1].astype(jnp.int32)


def rows_kernel(meta_ref, cur_ref, nxt_ref, code_ref, table, pooled, wp, x_out, g_buf, p_buf, sems, *, B, U, scale):
    i = pl.program_id(0)
    n = pl.num_programs(0)

    def issue(ref, slot):
        def start(k, s, img):
            src = (pooled if img else table).at[pl.ds(pl.multiple_of(s - IMG * img, 8), 8), :]
            dst = (p_buf if img else g_buf).at[slot, pl.ds(pl.multiple_of(k * 8, 8), 8), :]
            pltpu.make_async_copy(src, dst, sems.at[img, slot]).start()

        def body(kk, carry):
            src = [ref[0, kk * U + u] for u in range(U)]
            some = functools.reduce(jnp.bitwise_or, src) >= IMG
            every = functools.reduce(jnp.bitwise_and, src) >= IMG
            for img, alike in ((0, jnp.logical_not(some)), (1, every)):
                @pl.when(alike)
                def _():
                    for u, s in enumerate(src):
                        start(kk * U + u, s, img)

            @pl.when(some & jnp.logical_not(every))
            def _():
                def single(u, carry):
                    k = kk * U + u
                    s = ref[0, k]
                    for img in (0, 1):
                        @pl.when((s >= IMG) == bool(img))
                        def _():
                            start(k, s, img)
                    return carry

                lax.fori_loop(0, U, single, 0)
            return carry

        lax.fori_loop(0, B // U, body, 0)

    @pl.when(i == 0)
    def _():
        g_buf[...] = jnp.zeros_like(g_buf)
        p_buf[...] = jnp.zeros_like(p_buf)
        issue(cur_ref, 0)

    slot = lax.rem(i, 2)

    @pl.when(i + 1 < n)
    def _():
        issue(nxt_ref, 1 - slot)

    ni = cur_ref[3, 0]
    nt = B - ni

    @pl.when(nt > 0)
    def _():
        sz = pl.multiple_of(nt * 8, 8)
        pltpu.make_async_copy(table.at[pl.ds(0, sz), :], g_buf.at[slot, pl.ds(0, sz), :], sems.at[0, slot]).wait()

    @pl.when(ni > 0)
    def _():
        sz = pl.multiple_of(ni * 8, 8)
        pltpu.make_async_copy(pooled.at[pl.ds(0, sz), :], p_buf.at[slot, pl.ds(0, sz), :], sems.at[1, slot]).wait()

    code = as_column(code_ref[1:2, :])
    row = lax.broadcasted_iota(jnp.int32, (B, B * 8), 0)
    col = lax.broadcasted_iota(jnp.int32, (B, B * 8), 1)
    sel = jnp.where(col == row * 8 + (code & 7), 1.0, 0.0).astype(BF)

    def text():
        return (jnp.dot(sel, g_buf[slot], preferred_element_type=F32) * scale).astype(BF)

    def soft():
        picked = jnp.dot(sel, p_buf[slot], preferred_element_type=F32).astype(BF)
        return jnp.dot(picked, wp[...], preferred_element_type=F32).astype(BF)

    @pl.when(ni == 0)
    def _():
        x_out[...] = text()

    @pl.when(nt == 0)
    def _():
        x_out[...] = soft()

    @pl.when((ni > 0) & (nt > 0))
    def _():
        x_out[...] = jnp.where(code >= 8, soft(), text())


def build_rows(meta, idx, table, pooled, wp, scale, E):
    D = table.shape[1]
    V = pooled.shape[1]
    B = ROW_BLOCK
    last = idx.shape[1] // B - 1

    def at(ahead):
        return lambda i, meta: (0, jnp.clip(meta[0] // B - WINDOW // B + i + ahead, 0, last))

    return pl.pallas_call(
        functools.partial(rows_kernel, B=B, U=16, scale=scale),
        grid_spec=pltpu.PrefetchScalarGridSpec(
            num_scalar_prefetch=1, grid=(E // B,),
            in_specs=[pl.BlockSpec((8, B), at(0), memory_space=pltpu.SMEM), pl.BlockSpec((8, B), at(1), memory_space=pltpu.SMEM), pl.BlockSpec((8, B), at(0)),
                      ANY, ANY, whole((V, D))],
            out_specs=pl.BlockSpec((B, D), by_row),
            scratch_shapes=[pltpu.VMEM((2, B * 8, D), BF), pltpu.VMEM((2, B * 8, V), BF), DMA((2, 2))]),
        out_shape=like((E, D), BF),
        compiler_params=params(dimension_semantics=("arbitrary",)),
        cost_estimate=cost(E * (D + V) * 1024, E * D * 16),
        name="build_rows",
    )(meta, idx, idx, idx, table, pooled, wp)


def qkv_kernel(meta_ref, x_ref, near_ref, far_ref, n0_ref, qk_ref, *rest, q_lo, q_hi, nq, nk):
    *w_refs, q_out, k_out, v_out, w_buf, sem = rest
    i = pl.program_id(0)
    M = x_ref.shape[0]
    half = HD // 2

    @pl.when(i == 0)
    def _():
        copies = []
        if len(w_refs) == 3:
            for k, (ref, lo, hi) in enumerate(zip(w_refs, (0, nq, nq + nk), (nq, nq + nk, nq + 2 * nk))):
                copies.append(pltpu.make_async_copy(ref, w_buf.at[:, lo:hi], sem.at[k]))
        else:
            e = w_refs[0].shape[0]
            for k, ref in enumerate(w_refs):
                copies.append(pltpu.make_async_copy(ref, w_buf.at[pl.ds(pl.multiple_of(meta_ref[1 + k], e), e), :], sem.at[k]))
        for cp in copies:
            cp.start()
        for cp in copies:
            cp.wait()

    cos, sin = [], []
    cn, sn = near_ref[:, :half], near_ref[:, half:]
    for t in range(M // ROPE_STEP):
        far = far_ref[pl.ds(meta_ref[0] // ROPE_STEP + i * (M // ROPE_STEP) + t, 1), :]
        cf, sf = far[:, :half], far[:, half:]
        cos.append(cf * cn - sf * sn)
        sin.append(sf * cn + cf * sn)
    cos = jnp.concatenate(cos, axis=0)
    sin = jnp.concatenate(sin, axis=0)

    def work(first):
        a = normed(x_ref[...].astype(F32), n0_ref[...]).astype(BF)
        acc = jnp.dot(a, w_buf[:, first:], preferred_element_type=F32)

        def heads(col, count, oref, weight, post):
            for h in range(count):
                one = acc[:, col - first + h * HD:col - first + (h + 1) * HD]
                mean_sq = jnp.mean(one * one, axis=-1, keepdims=True)
                one = one * (lax.rsqrt(mean_sq + EPS) * post) * (1.0 + weight)
                lo = one[:, :half]
                hi = one[:, half:]
                oref[:, h * HD:h * HD + half] = (lo * cos - hi * sin).astype(BF)
                oref[:, h * HD + half:(h + 1) * HD] = (hi * cos + lo * sin).astype(BF)

        if first == 0:
            heads(0, nq // HD, q_out, qk_ref[0:1, :], HD ** -0.5)
        heads(nq, nk // HD, k_out, qk_ref[1:2, :], 1.0)
        v_out[...] = acc[:, nq + nk - first:].astype(BF)

    is_q = (i >= q_lo) & (i < q_hi)

    @pl.when(is_q)
    def _():
        work(0)

    @pl.when(jnp.logical_not(is_q))
    def _():
        work(nq)


def project_qkv(meta, x, near, far, n0, qk, weights, cols, *, rows, M=512):
    E, D = x.shape
    hq, hk = cols
    lo = WINDOW // M
    hi = (WINDOW + rows) // M
    return pl.pallas_call(
        functools.partial(qkv_kernel, q_lo=lo, q_hi=hi, nq=hq, nk=hk),
        grid_spec=pltpu.PrefetchScalarGridSpec(
            num_scalar_prefetch=1, grid=(pl.cdiv(E, M),),
            in_specs=[pl.BlockSpec((M, D), by_row), pl.BlockSpec(near.shape, fixed), pl.BlockSpec(far.shape, fixed), pl.BlockSpec((1, D), fixed), pl.BlockSpec((2, HD), fixed)]
            + [ANY] * len(weights),
            out_specs=[pl.BlockSpec((M, hq), lambda i, *_: (jnp.clip(i - lo, 0, hi - lo - 1), 0)), pl.BlockSpec((M, hk), by_row), pl.BlockSpec((M, hk), by_row)],
            scratch_shapes=[pltpu.VMEM((D, hq + 2 * hk), BF), DMA((4,))]),
        out_shape=[like((rows, hq), BF), like((E, hk), BF), like((E, hk), BF)],
        compiler_params=params(dimension_semantics=("arbitrary",)),
        cost_estimate=cost(D * (rows * hq + 2 * E * hk), E * D),
        name="project_qkv",
    )(meta, x, near, far, n0, qk, *weights)


def attn_kernel(meta_ref, q_ref, k_ref, v_ref, cur_ref, nxt_ref, cur_s, nxt_s, o_ref, *, BQ, last):
    i = pl.program_id(0)
    r0 = pl.multiple_of(i * BQ, BQ)
    first = meta_ref[0] - WINDOW + r0
    nw = WINDOW // BQ
    kv = k_ref.shape[1] // HD
    n = q_ref.shape[1] // HD
    row = lax.broadcasted_iota(jnp.int32, (BQ, BQ), 0)
    col = lax.broadcasted_iota(jnp.int32, (BQ, BQ), 1)
    idq = as_column(cur_ref[2:3, :])

    def attend(nb, edge):
        def bias(b):
            if 0 < b < nw and not edge:
                return None
            ok = None
            if b == 0:
                ok = row < col
            elif b >= nw:
                ok = (idq == (cur_ref if b == nw else nxt_ref)[2:3, :]) & (idq >= 0)
                if b == nw:
                    ok = ok | (row >= col)
            if edge and b < nw:
                inside = first + b * BQ >= 0
                ok = inside if ok is None else ok & inside
            return jnp.where(ok, 0.0, -1e30)

        biases = [bias(b) for b in range(nb)]

        def score(u):
            at = u * kv // n * HD
            return lax.dot_general(q_ref[:, u * HD:(u + 1) * HD], k_ref[pl.ds(r0, nb * BQ), at:at + HD], (((1,), (1,)), ((), ())), preferred_element_type=F32)

        def soft(s):
            parts = [s[:, b * BQ:(b + 1) * BQ] for b in range(nb)]
            parts = [p if m is None else p + m for p, m in zip(parts, biases)]
            top = functools.reduce(jnp.maximum, parts).max(axis=-1, keepdims=True)
            probs = [jnp.exp(p - top) for p in parts]
            inv = 1.0 / functools.reduce(jnp.add, probs).sum(axis=-1, keepdims=True)
            return jnp.concatenate([p.astype(BF) for p in probs], axis=1), inv

        scores = [score(u) for u in range(n)]
        soft_w = [soft(s) for s in scores]
        for u, (p, inv) in enumerate(soft_w):
            at = u * kv // n * HD
            o = jnp.dot(p, v_ref[pl.ds(r0, nb * BQ), at:at + HD], preferred_element_type=F32)
            o_ref[:, u * HD:(u + 1) * HD] = (o * inv).astype(BF)

    here = meta_ref[0] // BQ + i
    ahead = cur_s[2, BQ - 1]
    crosses = (ahead >= 0) & (ahead == nxt_s[2, 0]) & (here < last)

    @pl.when(first < 0)
    def _():
        attend(nw + 2, True)

    @pl.when((first >= 0) & crosses)
    def _():
        attend(nw + 2, False)

    @pl.when((first >= 0) & jnp.logical_not(crosses))
    def _():
        attend(nw + 1, False)


def attention(meta, q, k, v, idx, *, BQ=256):
    R, HQ = q.shape
    E, HK = k.shape
    span = WINDOW + BQ
    last = idx.shape[1] // BQ - 1

    def at(ahead):
        return lambda i, meta: (0, jnp.minimum(meta[0] // BQ + i + ahead, last))

    return pl.pallas_call(
        functools.partial(attn_kernel, BQ=BQ, last=last),
        grid_spec=pltpu.PrefetchScalarGridSpec(
            num_scalar_prefetch=1, grid=(R // BQ,),
            in_specs=[pl.BlockSpec((BQ, HQ), by_row), whole((E, HK)), whole((E, HK))]
            + [pl.BlockSpec((8, BQ), at(d)) for d in (0, 1)] + [pl.BlockSpec((8, BQ), at(d), memory_space=pltpu.SMEM) for d in (0, 1)],
            out_specs=pl.BlockSpec((BQ, HQ), by_row)),
        out_shape=like((R, HQ), BF),
        compiler_params=params(dimension_semantics=("arbitrary",)),
        cost_estimate=cost(2 * R * HQ * span, 4 * R * HQ),
        name="attention",
    )(meta, q, k, v, idx, idx, idx, idx)


def out_kernel(meta_ref, al_ref, ar_ref, x_ref, n1_ref, wl, *rest, sub):
    *pieces, h_out, w_buf, sem = rest
    K = wl.shape[0]

    @pl.when(pl.program_id(0) == 0)
    def _():
        e = pieces[0].shape[0]
        copies = [pltpu.make_async_copy(wl, w_buf.at[0:K, :], sem.at[4])]
        for k, ref in enumerate(pieces):
            copies.append(pltpu.make_async_copy(ref, w_buf.at[pl.ds(pl.multiple_of(K + meta_ref[5 + k], e), e), :], sem.at[k]))
        for cp in copies:
            cp.start()
        for cp in copies:
            cp.wait()

    blocks = [pl.ds(m * sub, sub) for m in range(al_ref.shape[0] // sub)]
    sums = [jnp.dot(al_ref[r, :], w_buf[0:K, :], preferred_element_type=F32) + jnp.dot(ar_ref[r, :], w_buf[K:, :], preferred_element_type=F32) for r in blocks]
    for r, o in zip(blocks, sums):
        post = normed(o.astype(BF).astype(F32), n1_ref[...]).astype(BF)
        h_out[r, :] = (x_ref[r, :].astype(F32) + post.astype(F32)).astype(BF)


def project_out(meta, al, ar, x, n1, wl, pieces, *, M=512, sub=128):
    R, K = al.shape
    D = wl.shape[1]
    off = WINDOW // M
    return pl.pallas_call(
        functools.partial(out_kernel, sub=sub),
        grid_spec=pltpu.PrefetchScalarGridSpec(
            num_scalar_prefetch=1, grid=(R // M,),
            in_specs=[pl.BlockSpec((M, K), by_row), pl.BlockSpec((M, K), by_row), pl.BlockSpec((M, D), lambda i, *_: (i + off, 0)), pl.BlockSpec((1, D), fixed)]
            + [ANY] * 5,
            out_specs=pl.BlockSpec((M, D), by_row),
            scratch_shapes=[pltpu.VMEM((2 * K, D), BF), DMA((5,))]),
        out_shape=like((R, D), BF),
        compiler_params=params(dimension_semantics=("arbitrary",)),
        cost_estimate=cost(2 * R * K * D, 4 * R * D),
        name="project_out",
    )(meta, al, ar, x, n1, wl, *pieces)


def ffn_kernel(meta_ref, h_ref, n2_ref, n3_ref, *rest, mode, n_loc, n_rem, H, sub, mid, start, got_at):
    rest = list(rest)
    local = [rest.pop(0) for _ in range(3)] if n_loc else None
    remote = [rest.pop(0) for _ in range(12)] if n_rem else None
    acc_in = rest.pop(0) if mode == "R" else None
    got = None if got_at is None else rest.pop(0)
    *rest, z_ref, act, acc, gb, ub, db, p_buf, w_sem, o_sem, a_sem, p_sem = rest
    if mode == "L":
        acc_out = rest[-1]
    else:
        part_ref, full_ref = rest[-2:]
    j = pl.program_id(0)
    S = n_loc + n_rem
    M, D = h_ref.shape

    bufs = (gb, ub, db)
    into_hidden, out_of_hidden = (0, 1), (2,)

    def block(ref, k, at):
        return ref.at[at, :] if k in out_of_hidden else ref.at[:, at]

    def fetch(jj, which):
        sl = lax.rem(jj, 2)

        def near():
            at = pl.ds(pl.multiple_of(jj * H, H), H)
            for k in which:
                pltpu.make_async_copy(block(local[k], k, at), bufs[k].at[sl], w_sem.at[sl, k]).start()

        def far():
            at = pl.ds(pl.multiple_of((jj - n_loc) * H, H), H)
            for k in which:
                for p in range(4):
                    quarter = pl.ds(pl.multiple_of(meta_ref[1 + p], D // 4), D // 4)
                    dst = bufs[k].at[sl, :, quarter] if k in out_of_hidden else bufs[k].at[sl, quarter, :]
                    pltpu.make_async_copy(block(remote[4 * k + p], k, at), dst, w_sem.at[sl, k]).start()

        split(jj, near, far)

    def arrive(sl, which):
        for k in which:
            pltpu.make_async_copy(bufs[k].at[sl], bufs[k].at[sl], w_sem.at[sl, k]).wait()

    def split(jj, near, far):
        if n_loc and n_rem:
            pl.when(jj < n_loc)(near)
            pl.when(jj >= n_loc)(far)
        else:
            (near if n_loc else far)()

    def rows(m):
        return pl.ds(pl.multiple_of(m * sub, sub), sub)

    def acc_load():
        return pltpu.make_async_copy(acc_in, acc, a_sem)

    slot = lax.rem(j, 2)

    @pl.when(j == 0)
    def _():
        fetch(0, into_hidden)

    @pl.when(j < S)
    def _():
        arrive(slot, into_hidden)

    @pl.when(j < S - 1)
    def _():
        fetch(j + 1, into_hidden)

    @pl.when(j < S)
    def _():
        fetch(j, out_of_hidden)

    if mode == "R":
        @pl.when(j == 0)
        def _():
            acc_load().start()

        @pl.when(j == 1)
        def _():
            acc_load().wait()

    @pl.when(j > 0)
    def _():
        arrive(1 - slot, out_of_hidden)

    for p in range(0 if got is None else got.shape[0] // PIECE):
        load = pltpu.make_async_copy(got.at[p * PIECE:(p + 1) * PIECE, :], p_buf, p_sem)
        to = full_ref.at[pl.ds(pl.multiple_of(meta_ref[10] + got_at + p * PIECE, PIECE), PIECE), :]
        store = pltpu.make_async_copy(p_buf, to, p_sem)
        at = 4 * p

        @pl.when(j == at + 1)
        def _():
            load.start()

        @pl.when(j == at + 3)
        def _():
            load.wait()
            store.start()

        @pl.when(j == at + 5)
        def _():
            store.wait()

    def hidden(z):
        g = jnp.dot(z, gb[slot], preferred_element_type=F32)
        u = jnp.dot(z, ub[slot], preferred_element_type=F32)
        return g, u

    def gate(gu):
        return (jax.nn.gelu(gu[0], approximate=True) * gu[1]).astype(BF)

    def down(r):
        return jnp.dot(act[r, :], db[1 - slot], preferred_element_type=F32)

    @pl.when(j == 0)
    def _():
        def one(m, carry):
            z = normed(h_ref[rows(m), :].astype(F32), n2_ref[...]).astype(BF)
            z_ref[rows(m), :] = z
            act[rows(m), :] = gate(hidden(z))
            if mode != "R":
                acc[rows(m), :] = jnp.zeros((sub, D), F32)
            return carry

        lax.fori_loop(0, M // sub, one, 0)

    @pl.when((j > 0) & (j < S))
    def _():
        def one(m, carry):
            r = pl.ds(pl.multiple_of(m * mid, mid), mid)
            gu = hidden(z_ref[r, :])
            acc[r, :] += down(r)
            act[r, :] = gate(gu)
            return carry

        if M == mid:
            one(0, 0)
        else:
            lax.fori_loop(0, M // mid, one, 0)

    @pl.when(j == S)
    def _():
        def puts(m):
            if mode == "L":
                return [pltpu.make_async_copy(acc.at[rows(m), :], acc_out.at[rows(m), :], o_sem.at[0, m])]
            base = pl.multiple_of(meta_ref[9] + start + m * sub, sub)
            return [pltpu.make_async_copy(z_ref.at[rows(m), :], ref, o_sem.at[k, m]) for k, ref in enumerate((part_ref.at[rows(m), :], full_ref.at[pl.ds(base, sub), :]))]

        def one(m, carry):
            total = acc[rows(m), :] + down(rows(m))
            if mode == "L":
                acc[rows(m), :] = total
            else:
                post = normed(total.astype(BF).astype(F32), n3_ref[...]).astype(BF)
                z_ref[rows(m), :] = (h_ref[rows(m), :].astype(F32) + post.astype(F32)).astype(BF)
            for p in puts(m):
                p.start()
            return carry

        lax.fori_loop(0, M // sub, one, 0)
        for m in range(M // sub):
            for p in puts(m):
                p.wait()


def feed_forward(mode, meta, h, n2, n3, wl, wr, acc_in, full, total, start, M, got=None, *, H=512):
    sub = min(M, 512)
    mid = M
    R, D = h.shape
    F = (wl or wr)[0].shape[1]
    n_loc = F // H if mode in "LF" else 0
    n_rem = F // H if mode in "RF" else 0
    S = n_loc + n_rem
    in_specs = [pl.BlockSpec((M, D), lambda j, *_: (start // M, 0)), pl.BlockSpec((1, D), fixed), pl.BlockSpec((1, D), fixed)]
    args = [meta, h, n2, n3]
    args += list(wl) if n_loc else []
    args += list(wr) if n_rem else []
    if mode == "R":
        args.append(acc_in)
    if got is not None:
        args.append(got[0])
    out_shape = [like((M, D), F32)] if mode == "L" else [like((M, D), BF), like((total, D), BF)]
    aliases = {}
    if mode != "L" and full is not None:
        aliases = {len(args): 1}
        args.append(full)
    in_specs += [ANY] * (len(args) - 4)
    nm = M // sub
    mult = S * H // F
    out = pl.pallas_call(
        functools.partial(ffn_kernel, mode=mode, n_loc=n_loc, n_rem=n_rem, H=H, sub=sub, mid=mid, start=start, got_at=got and got[1]),
        grid_spec=pltpu.PrefetchScalarGridSpec(
            num_scalar_prefetch=1, grid=(S + 1,), in_specs=in_specs, out_specs=[ANY] * len(out_shape),
            scratch_shapes=[pltpu.VMEM((M, D), BF), pltpu.VMEM((M, H), BF), pltpu.VMEM((M, D), F32), pltpu.VMEM((2, D, H), BF), pltpu.VMEM((2, D, H), BF), pltpu.VMEM((2, H, D), BF), pltpu.VMEM((PIECE, D), BF),
                            DMA((2, 3)), DMA((2, nm)), DMA, DMA]),
        out_shape=out_shape, input_output_aliases=aliases,
        compiler_params=params(dimension_semantics=("arbitrary",)),
        cost_estimate=cost(3 * M * D * F * mult, 6 * D * F),
        name="feed_forward_" + mode.lower(),
    )(*args)
    return out[0] if mode == "L" else out


ROPE_STEP = 64


def rope_tables(total):
    inv_freq = ROPE_BASE ** (np.arange(HD // 2) * -2.0 / HD)
    near = np.arange(ROPE_STEP)[:, None] * inv_freq
    far = np.arange(-WINDOW, total + WINDOW, ROPE_STEP)[:, None] * inv_freq
    return tuple(jnp.asarray(np.concatenate([np.cos(t), np.sin(t)], axis=1), F32) for t in (near, far))


PIECE = 512
FFN_SPLIT = (1024, 1024, 512)
FFN_CHUNKS = ((0, 1024), (1, 1024), (None, 512), (None, 512), (2, 512), (None, 512))


def solution(mesh):
    rows_spec = P(('dp', 'sp'))
    in_specs = (P(('dp', 'sp'), None, None), rows_spec, rows_spec, rows_spec, P('tp', None), P(), P(), P(), P(), P(None, 'tp'), P(None, 'tp'), P(None, 'tp'), P('tp', None), P(None, 'tp'), P(None, 'tp'), P('tp', None))
    n_sp = mesh.shape['sp']
    swap = [(i, 1 - i) for i in range(2)]
    x_swap = [(i, i ^ 2) for i in range(n_sp)]
    c_swap = [(i, i ^ 1) for i in range(n_sp)]

    def over_y(v):
        return lax.ppermute(v, 'tp', swap)

    def over_x(v):
        return lax.ppermute(v, 'sp', x_swap)

    def over_c(v):
        return lax.ppermute(v, 'sp', c_swap)

    def after(*values):
        return lax.optimization_barrier(values)

    def device_fn(feats, tokens, img_slot, img_id, embed, proj_norm, w_proj, norms, qk_norms, w_q, w_k, w_v, w_o, w_gate, w_up, w_down):
        sp = lax.axis_index('sp')
        tp = lax.axis_index('tp')
        shard = tokens.shape[0]
        R = shard // 2
        total = shard * n_sp
        d_model = embed.shape[1]
        E = WINDOW + R + SOFT

        origin = [sp, sp ^ 2, sp ^ 1, sp ^ 3]
        meta = jnp.stack([sp * shard + tp * R] + [o * (d_model // 4) for o in origin] + [o * (w_o.shape[0] // 4) for o in origin] + [tp * R, (1 - tp) * R]).astype(jnp.int32)
        cell = np.arange(POOL_K * PATCH_SIDE) % PATCH_SIDE // POOL_K
        pmat = jnp.asarray((np.arange(PATCH_SIDE // POOL_K)[:, None] == cell) / POOL_K ** 2, BF)
        n0, n1, n2, n3 = (norms[k:k + 1] for k in range(4))
        near, far = rope_tables(total)
        meta, n0, n1, n2, n3, idx = after(meta, n0, n1, n2, n3, index_rows(tokens, img_slot, img_id))
        table, pooled, idx, qkv_p, o_p, g_p, u_p, d_p = gather_inputs(
            feats, embed, proj_norm[None, :], pmat, idx, w_q, w_k, w_v, w_o, w_gate, w_up, w_down)

        with jax.named_scope("over_y"):
            yq, yo, yg, yu, yd = (over_y(v) for v in (qkv_p, o_p, g_p, u_p, d_p))

        scale = float(np.sqrt(np.float32(d_model)).astype(jnp.bfloat16))
        cols = (w_q.shape[1], w_k.shape[1])
        x = build_rows(meta, idx, table, pooled, w_proj, scale, E)
        x, yq, yo = after(x, yq, yo)
        xq, cq = over_x(yq), over_c(yq)
        xo, co = over_x(yo), over_c(yo)
        ql, kl, vl = project_qkv(meta, x, near, far, n0, qk_norms, (w_q, w_k, w_v), cols, rows=R)
        ql, kl, vl, xq = after(ql, kl, vl, xq)
        dq = over_c(xq)
        attn_l = attention(meta, ql, kl, vl, idx)
        attn_l, yg, dq, xo, cq, co = after(attn_l, yg, dq, xo, cq, co)
        xg, cg = over_x(yg), over_c(yg)
        do = over_c(xo)
        heads_r = project_qkv(meta, x, near, far, n0, qk_norms, (yq, xq, cq, dq), cols, rows=R)
        attn_r = attention(meta, *heads_r, idx)
        attn_r, yu, do = after(attn_r, yu, do)
        xu, cu = over_x(yu), over_c(yu)
        h = project_out(meta, attn_l, attn_r, x, n1, w_o, (yo, xo, co, do))
        h, xg, cg = after(h, xg, cg)
        dg = over_c(xg)

        wl = (w_gate, w_up, w_down)
        accs = []
        start = 0
        for k, M in enumerate(FFN_SPLIT):
            acc = feed_forward("L", meta, h, n2, n3, wl, None, None, None, shard, start, M)
            if k == 0:
                acc, h, yd, dg, cu = after(acc, h, yd, dg, cu)
                xd, cd = over_x(yd), over_c(yd)
            if k == 1:
                acc, h, xu = after(acc, h, xu)
                du = over_c(xu)
            if k == len(FFN_SPLIT) - 1:
                acc, h, xd, cd, du = after(acc, h, xd, cd, du)
                dd = over_c(xd)
            accs.append((acc, start))
            start += M
        wr = (yg, xg, cg, dg, yu, xu, cu, du, yd, xd, cd, dd)

        full = None
        pending = []
        for k, M in FFN_CHUNKS:
            if k is None:
                at, acc, mode = start, None, "F"
                start += M
            else:
                (acc, at), mode = accs[k], "R"
            got = pending.pop(0) if len(pending) > 2 else None
            part, full = feed_forward(mode, meta, h, n2, n3, wl if mode == "F" else None, wr, acc, full, shard, at, M, got)
            pending.append((over_y(part), at))
        for got, at in pending:
            full = lax.dynamic_update_slice_in_dim(full, got, (1 - tp) * R + at, 0)
        return full

    return jax.shard_map(device_fn, mesh=mesh, in_specs=in_specs, out_specs=P(('dp', 'sp'), None), check_vma=False)
```
